32 devices in a mesh: gx: 4 (over y, x), gy: 2 (over core), gz: 4 (over z).
Axes of the slice: x: 2, y: 2, z: 4, core: 2. Of those that a mesh axis runs over, the one named last changes fastest.
Arguments:
- conserved: float32 [5, 64, 32, 512], P(None, 'gx', 'gy', 'gz'), as said below
Outputs:
- advanced: float32 [5, 64, 32, 512], P(None, 'gx', 'gy', 'gz')
Inputs may be any that keep to these rules, and one draw needn't show every extreme that they name: `conserved`: every cell has positive density and positive pressure (energy above the kinetic energy).
All inputs are finite; a program needn't handle non-finite values. Where the reference program divides by a largest or mean magnitude, that divisor is 1e-20 or more.
Results may differ from the reference program's by a relative error of at most 0.000066.
Values sent between devices are 32-bit elements; how exact they have to be, the bound alone decides.
A program may use at most 64 MiB of HBM per device.

```python
import jax
import jax.numpy as jnp
from jax import lax

NX = 64
NY = 32
NZ = 512


def draw_conserved(key, part):
    subkeys = jax.random.split(key, 3)
    grid_shape = (NX, NY, NZ)
    log_density = jax.random.uniform(subkeys[0], grid_shape, jnp.float32, -0.7, 0.7)
    log_pressure = jax.random.uniform(subkeys[1], grid_shape, jnp.float32, -0.7, 0.7)
    position = jnp.arange(NX, dtype=jnp.float32) / NX
    vel_scale = (0.3 + 0.6 * position)[:, None, None]
    velocity = jax.random.truncated_normal(subkeys[2], -4.0, 4.0, (3,) + grid_shape, jnp.float32) * vel_scale
    density = jnp.exp(log_density)
    pressure = jnp.exp(log_pressure)
    momentum = density * velocity
    energy = pressure / 0.4 + 0.5 * density * jnp.sum(velocity * velocity, axis=0)
    return jnp.stack([density, momentum[0], momentum[1], momentum[2], energy]).astype(jnp.float32)


def setup_inputs(seed: int = 0) -> dict:
    key_list = jax.random.split(jax.random.key(seed), 2)
    return {
        "conserved": draw_conserved(jax.random.fold_in(key_list[1], 71), 0),
    }


gamma_gas = 1.4
weno_eps = 1e-06
courant = 0.4

def primitives(components):
    density = components[0]
    vel_normal = components[1] / density
    vel_first = components[2] / density
    vel_second = components[3] / density
    kinetic = 0.5 * (vel_normal * vel_normal + vel_first * vel_first + vel_second * vel_second)
    pressure = (gamma_gas - 1.0) * (components[4] - density * kinetic)
    return (density, vel_normal, vel_first, vel_second, kinetic, pressure)

def multiply_rows(matrix, vector):
    result = []
    for matrix_row in matrix:
        accum = None
        for coefficient, component in zip(matrix_row, vector):
            if coefficient is None:
                continue
            product_term = component * coefficient
            accum = product_term if accum is None else accum + product_term
        result.append(accum)
    return result

def weno_face(far_left, near_left, centre, near_right, far_right):
    poly_left = (2.0 * far_left - 7.0 * near_left + 11.0 * centre) / 6.0
    poly_mid = (-near_left + 5.0 * centre + 2.0 * near_right) / 6.0
    poly_right = (2.0 * centre + 5.0 * near_right - far_right) / 6.0
    diff_one = far_left - 2.0 * near_left + centre
    diff_two = far_left - 4.0 * near_left + 3.0 * centre
    smooth_left = 13.0 / 12.0 * diff_one * diff_one + 0.25 * diff_two * diff_two
    diff_one = near_left - 2.0 * centre + near_right
    diff_two = near_left - near_right
    smooth_mid = 13.0 / 12.0 * diff_one * diff_one + 0.25 * diff_two * diff_two
    diff_one = centre - 2.0 * near_right + far_right
    diff_two = 3.0 * centre - 4.0 * near_right + far_right
    smooth_right = 13.0 / 12.0 * diff_one * diff_one + 0.25 * diff_two * diff_two
    weight_left = 0.1 / ((weno_eps + smooth_left) * (weno_eps + smooth_left))
    weight_mid = 0.6 / ((weno_eps + smooth_mid) * (weno_eps + smooth_mid))
    weight_right = 0.3 / ((weno_eps + smooth_right) * (weno_eps + smooth_right))
    return (weight_left * poly_left + weight_mid * poly_mid + weight_right * poly_right) / (weight_left + weight_mid + weight_right)

def face_divergence(components, line_axis, wave_speed, cell_count):
    length = components[0].shape[line_axis] - 6
    face_count = length + 1

    def window(array_item, start, count):
        return lax.slice_in_dim(array_item, start, start + count, axis=line_axis)
    density, vel_normal, vel_first, vel_second, kinetic, pressure = primitives(components)
    fluxes = [components[1], components[1] * vel_normal + pressure, components[2] * vel_normal, components[3] * vel_normal, (components[4] + pressure) * vel_normal]
    split_plus = [0.5 * (flux + wave_speed * component) for flux, component in zip(fluxes, components)]
    split_minus = [0.5 * (flux - wave_speed * component) for flux, component in zip(fluxes, components)]
    face_mean = [0.5 * (window(component, 2, face_count) + window(component, 3, face_count)) for component in components]
    mean_density, mean_normal, mean_first, mean_second, mean_kinetic, mean_pressure = primitives(face_mean)
    enthalpy = (face_mean[4] + mean_pressure) / mean_density
    sound_speed = jnp.sqrt(gamma_gas * mean_pressure / mean_density)
    inv_sound = 1.0 / sound_speed
    coef_one = (gamma_gas - 1.0) / (sound_speed * sound_speed)
    coef_two = coef_one * mean_kinetic
    left_rows = [[0.5 * (coef_two + mean_normal * inv_sound), -0.5 * (coef_one * mean_normal + inv_sound), -0.5 * coef_one * mean_first, -0.5 * coef_one * mean_second, 0.5 * coef_one], [-mean_first, None, 1.0, None, None], [-mean_second, None, None, 1.0, None], [1.0 - coef_two, coef_one * mean_normal, coef_one * mean_first, coef_one * mean_second, -coef_one], [0.5 * (coef_two - mean_normal * inv_sound), -0.5 * (coef_one * mean_normal - inv_sound), -0.5 * coef_one * mean_first, -0.5 * coef_one * mean_second, 0.5 * coef_one]]
    right_cols = [[1.0, None, None, 1.0, 1.0], [mean_normal - sound_speed, None, None, mean_normal, mean_normal + sound_speed], [mean_first, 1.0, None, mean_first, mean_first], [mean_second, None, 1.0, mean_second, mean_second], [enthalpy - mean_normal * sound_speed, mean_first, mean_second, mean_kinetic, enthalpy + mean_normal * sound_speed]]
    positive = [multiply_rows(left_rows, [window(component, offset, face_count) for component in split_plus]) for offset in range(5)]
    negative = [multiply_rows(left_rows, [window(component, offset, face_count) for component in split_minus]) for offset in range(1, 6)]
    wave_sums = []
    for wave_index in range(5):
        upwind = weno_face(*[positive[offset][wave_index] for offset in range(5)])
        downwind = weno_face(*[negative[offset][wave_index] for offset in (4, 3, 2, 1, 0)])
        wave_sums.append(upwind + downwind)
    face_flux = multiply_rows(right_cols, wave_sums)
    return [-(window(flux, 1, length) - window(flux, 0, length)) * cell_count for flux in face_flux]

def component_order(direction):
    if direction == 0:
        return [0, 1, 2, 3, 4]
    if direction == 1:
        return [0, 2, 1, 3, 4]
    return [0, 3, 1, 2, 4]

def direction_terms(padded_slab, line_axis, direction, wave_speed, cell_count):
    comp_order = component_order(direction)
    result = face_divergence([padded_slab[index] for index in comp_order], line_axis, wave_speed, cell_count)
    placed = [None] * 5
    for index, target in enumerate(comp_order):
        placed[target] = result[index]
    return jnp.stack(placed)

def reference(conserved):
    components = [conserved[index] for index in range(5)]
    density, vel_one, vel_two, vel_three, kinetic, pressure = primitives(components)
    sound_speed = jnp.sqrt(gamma_gas * pressure / density)
    speed_x = jnp.max(jnp.abs(vel_one) + sound_speed)
    speed_y = jnp.max(jnp.abs(vel_two) + sound_speed)
    speed_z = jnp.max(jnp.abs(vel_three) + sound_speed)
    step = courant / (speed_x * NX + speed_y * NY + speed_z * NZ)
    padded = jnp.pad(conserved, ((0, 0), (3, 3), (0, 0), (0, 0)), mode='wrap')
    moved = jnp.moveaxis(padded, 2, 0)
    result = lax.map(lambda slab_item: direction_terms(slab_item, 0, 0, speed_x, NX), moved)
    tendency = jnp.moveaxis(result, 0, 2)
    padded = jnp.pad(conserved, ((0, 0), (0, 0), (3, 3), (0, 0)), mode='wrap')
    moved = jnp.moveaxis(padded, 1, 0)
    result = lax.map(lambda slab_item: direction_terms(slab_item, 0, 1, speed_y, NY), moved)
    tendency = tendency + jnp.moveaxis(result, 0, 1)
    padded = jnp.pad(conserved, ((0, 0), (0, 0), (0, 0), (3, 3)), mode='wrap')
    moved = jnp.moveaxis(padded, 1, 0)
    result = lax.map(lambda slab_item: direction_terms(slab_item, 1, 2, speed_z, NZ), moved)
    tendency = tendency + jnp.moveaxis(result, 0, 1)
    return conserved + step * tendency
```

```python
import functools
import itertools

import jax
import jax.numpy as jnp
from jax import lax
from jax.experimental import pallas as pl
from jax.experimental.pallas import tpu as pltpu
from jax.sharding import PartitionSpec as P

GAMMA = 1.4
EPS = 1e-06 * (3.0 / 16.0)
COURANT = 0.4
MESH = pl.DeviceIdType.MESH
AXES = ("gx", "gy", "gz")
ORDERS = ([0, 1, 2, 3, 4], [0, 2, 1, 3, 4], [0, 3, 1, 2, 4])
LANES = 128
FIELD = 12
STATE = 5 * FIELD
LINEAR = STATE + 6
KEPT = LINEAR + 10


def project(u, vn, va, vb, kin, b1h, ich):
    a = u[4] + kin * u[0] - vn * u[1] - va * u[2] - vb * u[3]
    a = b1h * a
    b = (vn * u[0] - u[1]) * ich
    return [a + b, u[2] - va * u[0], u[3] - vb * u[0], u[0] - (a + a), a - b]


def nonlinear(e1, e2, e3, h):
    c = ((4.0 / 3.0) * h) * h + EPS
    g = h + 0.75 * e2
    q0 = 1.0 / (e1 * (e1 + h) + c)
    q1 = 1.0 / (e2 * (e2 + h) + c)
    q2 = 1.0 / (e3 * (e3 - g) + (((4.0 / 3.0) * g) * g + EPS))
    w0 = q0 * q0
    w2 = 3.0 * (q2 * q2)
    n0 = e1 - e2
    return (w0 * (n0 + n0) + w2 * (e2 - e3)) / (w0 + w2 + 6.0 * (q1 * q1))


def rows_of(j):
    return pl.ds(pl.multiple_of(8 * j, 8), 8)


class Sweep:
    def __init__(self, direction, slots, lane_rows, q, work, kept):
        self.order = ORDERS[direction]
        self.slots, self.r = slots, lane_rows
        self.q, self.work, self.kept = q, work, kept

    def cell(self, j):
        s = [self.q[c, rows_of(j), :] for c in self.order]
        inv = 1.0 / s[0]
        vq = s[1] * (0.25 * inv)
        pq = 0.25 * (GAMMA - 1.0) * (s[4] - (0.5 * inv) * (s[1] * s[1] + s[2] * s[2] + s[3] * s[3]))
        f = [0.25 * s[1], s[1] * vq + pq, s[2] * vq, s[3] * vq, s[4] * vq + 4.0 * (pq * vq)]
        for c in range(5):
            self.work[j, c] = f[c]

    def differ(self, j):
        r = self.r
        for c in range(5):
            flux = [self.work[j + k * r, c] for k in (-1, 0, 1)]
            state = [self.q[self.order[c], rows_of(j + k * r), :] for k in (-1, 0, 1)]
            for place, (low, mid, high) in ((5, flux), (10, state)):
                below = mid - low
                self.work[j, place + c] = (high - mid) - below
                self.work[j, place + 10 + c] = 0.75 * below

    def face(self, j):
        q, work, kept, r = self.q, self.work, self.kept, self.r
        mean = [q[c, rows_of(j + 2 * r), :] + q[c, rows_of(j + 3 * r), :] for c in self.order]
        inv = 1.0 / mean[0]
        vn, va, vb = mean[1] * inv, mean[2] * inv, mean[3] * inv
        kin = 0.5 * (vn * vn + va * va + vb * vb)
        c2 = GAMMA * (GAMMA - 1.0) * (mean[4] * inv - kin)
        ic = lax.rsqrt(c2)
        args = (vn, va, vb, kin, (0.5 * (GAMMA - 1.0)) * (ic * ic), 0.5 * ic)
        state = (vn, va, vb, kin, c2 * ic, (1.0 / (GAMMA - 1.0)) * c2 + kin)
        for k in range(6):
            kept[j, STATE + k] = state[k]
        places = [(k, 5, k - 1) for k in (1, 2, 3, 4)] + [(k, 10, k + 3) for k in (1, 2, 3, 4)]
        places += [(2, 15, 8), (4, 15, 9), (2, 20, 10), (4, 20, 11)]
        for cell, place, slot in places:
            u = project([work[j + cell * r, place + c] for c in range(5)], *args)
            for k in range(5):
                kept[j, FIELD * k + slot] = u[k]
        for c in range(5):
            near, far = work[j + 2 * r, c], work[j + 3 * r, c]
            kept[j, LINEAR + c] = 6.0 * (near + far) - work[j + 2 * r, 5 + c] - work[j + 3 * r, 5 + c]
            kept[j, LINEAR + 5 + c] = work[j + 3 * r, 10 + c] - work[j + 2 * r, 10 + c]

    def run(self, step, low, high, unroll=1):
        def body(t, _):
            step(t + low * self.r)
            return 0

        lax.fori_loop(0, (high - low) * self.r, body, 0, unroll=unroll)

    def run_two(self, step, low, high, width, unroll=1):
        def body(t, _):
            step(t + low * self.r + (t // (width * self.r)) * ((high - low - width) * self.r))
            return 0

        lax.fori_loop(0, 2 * width * self.r, body, 0, unroll=unroll)

    def inside(self):
        n = self.slots
        self.run(self.cell, 3, n + 3, 2)
        self.run(self.differ, 4, n + 2, 2)
        self.run(self.face, 3, n - 2)

    def outside(self):
        n = self.slots
        self.run_two(self.cell, 0, n + 3, 3, 2)
        self.run_two(self.differ, 1, n + 2, 3, 2)
        self.run_two(self.face, 0, n - 2, 3)


def face_flux(order, quarter, kept, j):
    n = []
    for k in range(5):
        a1, a2, a3, a4, b1, b2, b3, b4, ha, hb, sa, sb = (kept[j, FIELD * k + i] for i in range(FIELD))
        t2, t3 = quarter * b2, quarter * b3
        left = nonlinear(a1 + quarter * b1, a2 + t2, a3 + t3, ha + quarter * sa)
        right = nonlinear(a4 - quarter * b4, a3 - t3, a2 - t2, quarter * sb - hb)
        n.append(left + right)
    vn, va, vb, kin, sound, enthalpy = (kept[j, STATE + i] for i in range(6))
    d = sound * (n[4] - n[0])
    s15 = n[0] + n[4]
    s = s15 + n[3]
    out = [
        s,
        vn * s + d,
        va * s + n[1],
        vb * s + n[2],
        enthalpy * s15 + vn * d + va * n[1] + vb * n[2] + kin * n[3],
    ]
    flux = [None] * 5
    for c in range(5):
        flux[order[c]] = (kept[j, LINEAR + c] + quarter * kept[j, LINEAR + 5 + c]) + out[c]
    return flux


def gather_kernel(
    sizes, stages, shape, cons_hbm, cons, kept_x, kept_y, kept_z, speeds, qx, qy, qz, wx, wy, wz,
    xh, yh, zh, ysend, zsend, mine, theirs, halo_send, halo_recv, max_send, max_recv, load_sem,
):
    lx, ly, lz = shape
    rows = lx * ly
    groups = rows // LANES
    blocks = 8 // groups
    inner = lz // blocks
    load = pltpu.make_async_copy(cons_hbm, cons, load_sem)
    load.start()
    here = [lax.axis_index(axis) for axis in AXES]
    peers = []
    for axes in stages:
        group = []
        for shift in itertools.product(*[range(sizes[a]) for a in axes]):
            if any(shift):
                group.append({AXES[a]: lax.rem(here[a] + k, sizes[a]) for a, k in zip(axes, shift)})
        peers.append(group)
    barrier = pltpu.get_barrier_semaphore()
    count = 0
    for group in peers:
        for peer in group:
            pl.semaphore_signal(barrier, inc=1, device_id=peer, device_id_type=MESH)
            count += 1
    load.wait()

    best = [None] * 3
    for j in range(rows // 8):
        q = [cons[c, pl.ds(8 * j, 8), :] for c in range(5)]
        inv = 1.0 / q[0]
        vel = [q[d] * inv for d in (1, 2, 3)]
        kinetic = 0.5 * (vel[0] * vel[0] + vel[1] * vel[1] + vel[2] * vel[2])
        sound = jnp.sqrt((GAMMA * (GAMMA - 1.0)) * (q[4] * inv - kinetic))
        for d in range(3):
            value = jnp.abs(vel[d]) + sound
            best[d] = value if best[d] is None else jnp.maximum(best[d], value)
    for d in range(3):
        mine[0, pl.ds(d, 1), :] = jnp.max(best[d], axis=0, keepdims=True)
    mine[0, pl.ds(3, 5), :] = jnp.zeros((5, LANES), jnp.float32)

    for c in range(5):
        for k in range(3):
            ysend[0, c, pl.ds(k * lx, lx), :] = cons[c, pl.ds(ly - 3 + k, lx, stride=ly), :]
            ysend[1, c, pl.ds(k * lx, lx), :] = cons[c, pl.ds(k, lx, stride=ly), :]
    for c in range(5):
        for g in range(groups):
            turned = jnp.transpose(cons[c, pl.ds(g * LANES, LANES), :])
            for b in range(blocks):
                qz[c, pl.ds(24 + b * groups + g, inner, stride=8), :] = turned[b * inner:(b + 1) * inner]
            for k in range(3):
                zsend[0, c, k, g:g + 1, :] = turned[lz - 3 + k:lz - 2 + k]
                zsend[1, c, k, g:g + 1, :] = turned[k:k + 1]
    x_edge, y_edge = 3 * ly, 3 * lx
    for c in range(5):
        for y in range(ly):
            qy[c, pl.ds(y_edge + y * lx, lx), :] = cons[c, pl.ds(y, lx, stride=ly), :]
    qx[:, pl.ds(x_edge, rows), :] = cons[...]

    along = [
        Sweep(0, lx, ly // 8, qx, wx, kept_x),
        Sweep(1, ly, lx // 8, qy, wy, kept_y),
        Sweep(2, inner, 1, qz, wz, kept_z),
    ]
    along[1].inside()

    def halo(slot, src, dst, axis, up):
        me, size = here[axis], sizes[axis]
        target = lax.rem(me + (1 if up else size - 1), size)
        return pltpu.make_async_remote_copy(
            src_ref=src, dst_ref=dst, send_sem=halo_send.at[slot], recv_sem=halo_recv.at[slot],
            device_id={AXES[axis]: target}, device_id_type=MESH,
        )

    def spread(stage):
        copies = []
        first = sum(len(group) for group in peers[:stage])
        for k, peer in enumerate(peers[stage]):
            slot = first + k
            copy = pltpu.make_async_remote_copy(
                src_ref=mine.at[stage], dst_ref=theirs.at[slot],
                send_sem=max_send.at[slot], recv_sem=max_recv.at[slot],
                device_id=peer, device_id_type=MESH,
            )
            copy.start()
            copies.append((slot, copy))
        return copies

    def gather(stage, copies):
        value = mine[stage]
        for slot, copy in copies:
            copy.wait_recv()
            value = jnp.maximum(value, theirs[slot])
        return value

    pl.semaphore_wait(barrier, count)
    sent = [spread(0)]
    halos = [
        [
            halo(0, cons.at[:, pl.ds(rows - x_edge, x_edge), :], xh.at[0], 0, True),
            halo(1, cons.at[:, pl.ds(0, x_edge), :], xh.at[1], 0, False),
        ],
        [halo(2, ysend.at[0], yh.at[0], 1, True), halo(3, ysend.at[1], yh.at[1], 1, False)],
        [halo(4, zsend.at[0], zh.at[0], 2, True), halo(5, zsend.at[1], zh.at[1], 2, False)],
    ]
    for axis in (2, 1, 0):
        for copy in halos[axis]:
            copy.start()

    def fill_y():
        for copy in halos[1]:
            copy.wait()
        qy[:, pl.ds(0, y_edge), :] = yh[0]
        qy[:, pl.ds(y_edge + rows, y_edge), :] = yh[1]
        along[1].outside()

    def fill_z():
        for copy in halos[2]:
            copy.wait()
        size = inner * 8
        for c in range(5):
            for k in range(3):
                low, high = 8 * k, 24 + size + 8 * k
                qz[c, low:low + groups, :] = zh[0, c, k]
                qz[c, low + groups:low + 8, :] = qz[c, size + 8 * k:size + 8 + 8 * k - groups, :]
                qz[c, high:high + 8 - groups, :] = qz[c, 24 + 8 * k + groups:32 + 8 * k, :]
                qz[c, high + 8 - groups:high + 8, :] = zh[1, c, k]
        along[2].outside()

    def fill_x():
        for copy in halos[0]:
            copy.wait()
        qx[:, pl.ds(0, x_edge), :] = xh[0]
        qx[:, pl.ds(x_edge + rows, x_edge), :] = xh[1]
        along[0].outside()

    work = [along[2].inside, along[0].inside]
    work.pop(0)()
    for stage in range(1, len(stages)):
        mine[stage] = gather(stage - 1, sent[-1])
        sent.append(spread(stage))
        if work:
            work.pop(0)()
    for rest in work:
        rest()
    fill_y()
    fill_z()
    top = gather(len(stages) - 1, sent[-1])
    for copies in sent:
        for _, copy in copies:
            copy.wait_send()
    for d in range(3):
        largest = jnp.max(top[d:d + 1], axis=1, keepdims=True)
        speeds[d] = jnp.broadcast_to(largest, (8, LANES))
    fill_x()


def combine_kernel(
    cells, shape, cons, kept_x, kept_y, kept_z, speeds, out_hbm, tend, acc, out, tz, faces, store_sem,
):
    lx, ly, lz = shape
    rows = lx * ly
    groups = rows // LANES
    blocks = 8 // groups
    inner = lz // blocks
    speed = [speeds[d] for d in range(3)]
    step = COURANT / (speed[0] * cells[0] + speed[1] * cells[1] + speed[2] * cells[2])
    quarter = [0.25 * speed[d] for d in range(3)]
    scale = [step * (cells[d] / 3.0) for d in range(3)]

    def sweep(direction, r, kept, flux, place, low, high):
        def body(j, _):
            new = face_flux(ORDERS[direction], quarter[direction], kept, j)
            old = [flux[j, c] for c in range(5)]
            for c in range(5):
                flux[j + r, c] = new[c]
            for c in range(5):
                place(j, c, scale[direction] * (old[c] - new[c]))
            return 0

        lax.fori_loop(low * r, high * r, body, 0)

    ry, rx = lx // 8, ly // 8

    def place_y(j, c, value):
        y = jnp.maximum(j // ry - 1, 0)
        tend[c, pl.ds(8 * ly * (j % ry) + y, 8, stride=ly), :] = value

    def place_z(j, c, value):
        tz[c, rows_of(jnp.maximum(j - 1, 0)), :] = value

    def place_x(j, c, value):
        x = jnp.maximum(j // rx - 1, 0)
        here = rows_of(x * rx + j % rx)
        out[c, here, :] = acc[c, here, :] + value

    sweep(1, ry, kept_y, faces, place_y, 0, ly + 1)
    sweep(2, 1, kept_z, faces, place_z, 0, inner + 1)
    for c in range(5):
        for g in range(groups):
            parts = [tz[c, pl.ds(b * groups + g, inner, stride=8), :] for b in range(blocks)]
            turned = jnp.transpose(jnp.concatenate(parts, axis=0))
            here = pl.ds(g * LANES, LANES)
            acc[c, here, :] = (cons[c, here, :] + tend[c, here, :]) + turned
    stores = []
    chunk = lx // 4
    for m in range(4):
        sweep(0, rx, kept_x, faces, place_x, 0 if m == 0 else m * chunk + 1, (m + 1) * chunk + 1)
        part = pl.ds(m * chunk * ly, chunk * ly)
        stores.append(pltpu.make_async_copy(out.at[:, part, :], out_hbm.at[:, part, :], store_sem.at[m]))
        stores[-1].start()
    for store in stores:
        store.wait()


def solution(mesh):
    sizes = [mesh.shape[axis] for axis in AXES]
    stages = [(0, 1), (2,)] if sizes[0] * sizes[1] <= 16 else [(0,), (2,), (1,)]

    def per_device(conserved):
        _, lx, ly, lz = conserved.shape
        shape = (lx, ly, lz)
        cells = [float(n * s) for n, s in zip(shape, sizes)]
        rows = lx * ly
        groups = rows // LANES
        inner = lz * groups // 8
        assert lz == LANES and rows % LANES == 0 and 8 % groups == 0 and lx % 8 == 0 and ly % 8 == 0
        total = 0
        for axes in stages:
            size = 1
            for a in axes:
                size *= sizes[a]
            total += size - 1

        def vmem(*dims):
            return pltpu.VMEM(dims, jnp.float32)

        def faces(count):
            return vmem(count, KEPT, 8, LANES)

        pads = [(lx + 6) * ly // 8, (ly + 6) * lx // 8, inner + 6]
        kept = [faces((lx + 1) * ly // 8), faces((ly + 1) * lx // 8), faces(inner + 1)]
        whole = pl.BlockSpec(memory_space=pltpu.VMEM)
        cons, kept_x, kept_y, kept_z, speeds = pl.pallas_call(
            functools.partial(gather_kernel, sizes, stages, shape),
            name="gather",
            out_shape=[vmem(5, rows, lz)] + kept + [vmem(3, 8, LANES)],
            in_specs=[pl.BlockSpec(memory_space=pltpu.HBM)],
            out_specs=[whole] * 5,
            scratch_shapes=[vmem(5, 8 * n, LANES) for n in pads] + [vmem(n, 25, 8, LANES) for n in pads] + [
                vmem(2, 5, 3 * ly, lz),
                vmem(2, 5, 3 * lx, lz),
                vmem(2, 5, 3, groups, LANES),
                vmem(2, 5, 3 * lx, lz),
                vmem(2, 5, 3, groups, LANES),
                vmem(len(stages), 8, LANES),
                vmem(total, 8, LANES),
                pltpu.SemaphoreType.DMA((6,)),
                pltpu.SemaphoreType.DMA((6,)),
                pltpu.SemaphoreType.DMA((total,)),
                pltpu.SemaphoreType.DMA((total,)),
                pltpu.SemaphoreType.DMA,
            ],
            compiler_params=pltpu.CompilerParams(
                collective_id=0, has_side_effects=True, vmem_limit_bytes=18 * 2**20
            ),
        )(pltpu.with_memory_space_constraint(conserved.reshape(5, rows, lz), pltpu.HBM))
        out = pl.pallas_call(
            functools.partial(combine_kernel, cells, shape),
            name="combine",
            out_shape=jax.ShapeDtypeStruct((5, rows, lz), jnp.float32),
            in_specs=[whole] * 5,
            out_specs=pl.BlockSpec(memory_space=pl.ANY),
            scratch_shapes=[vmem(5, rows, lz)] * 3 + [
                vmem(5, 8 * inner, LANES),
                vmem(max((lx + 2) * ly // 8, (ly + 2) * lx // 8, inner + 2), 5, 8, LANES),
                pltpu.SemaphoreType.DMA((4,)),
            ],
            compiler_params=pltpu.CompilerParams(vmem_limit_bytes=16 * 2**20),
        )(cons, kept_x, kept_y, kept_z, speeds)
        return out.reshape(conserved.shape)

    return jax.shard_map(
        per_device,
        mesh=mesh,
        in_specs=(P(None, "gx", "gy", "gz"),),
        out_specs=P(None, "gx", "gy", "gz"),
        check_vma=False,
    )
```

```python
import functools
import itertools

import jax
import jax.numpy as jnp
from jax import lax
from jax.experimental import pallas as pl
from jax.experimental.pallas import tpu as pltpu
from jax.sharding import PartitionSpec as P

GAMMA = 1.4
EPS = 1e-06 * (3.0 / 16.0)
COURANT = 0.4
MESH = pl.DeviceIdType.MESH
AXES = ("gx", "gy", "gz")
ORDERS = ([0, 1, 2, 3, 4], [0, 2, 1, 3, 4], [0, 3, 1, 2, 4])
LANES = 128
FIELD = 12
STATE = 5 * FIELD
LINEAR = STATE + 6
KEPT = LINEAR + 10


def project(u, vn, va, vb, kin, b1h, ich):
    a = u[4] + kin * u[0] - vn * u[1] - va * u[2] - vb * u[3]
    a = b1h * a
    b = (vn * u[0] - u[1]) * ich
    return [a + b, u[2] - va * u[0], u[3] - vb * u[0], u[0] - (a + a), a - b]


def nonlinear(e1, e2, e3, h):
    c = ((4.0 / 3.0) * h) * h + EPS
    g = h + 0.75 * e2
    q0 = 1.0 / (e1 * (e1 + h) + c)
    q1 = 1.0 / (e2 * (e2 + h) + c)
    q2 = 1.0 / (e3 * (e3 - g) + (((4.0 / 3.0) * g) * g + EPS))
    w0 = q0 * q0
    w2 = 3.0 * (q2 * q2)
    n0 = e1 - e2
    return (w0 * (n0 + n0) + w2 * (e2 - e3)) / (w0 + w2 + 6.0 * (q1 * q1))


def rows_of(j):
    return pl.ds(pl.multiple_of(8 * j, 8), 8)


class Sweep:
    def __init__(self, direction, slots, lane_rows, q, work, kept):
        self.order = ORDERS[direction]
        self.slots, self.r = slots, lane_rows
        self.q, self.work, self.kept = q, work, kept

    def cell(self, j):
        s = [self.q[c, rows_of(j), :] for c in self.order]
        inv = 1.0 / s[0]
        vq = s[1] * (0.25 * inv)
        pq = 0.25 * (GAMMA - 1.0) * (s[4] - (0.5 * inv) * (s[1] * s[1] + s[2] * s[2] + s[3] * s[3]))
        f = [0.25 * s[1], s[1] * vq + pq, s[2] * vq, s[3] * vq, s[4] * vq + 4.0 * (pq * vq)]
        for c in range(5):
            self.work[j, c] = f[c]

    def differ(self, j):
        r = self.r
        for c in range(5):
            flux = [self.work[j + k * r, c] for k in (-1, 0, 1)]
            state = [self.q[self.order[c], rows_of(j + k * r), :] for k in (-1, 0, 1)]
            for place, (low, mid, high) in ((5, flux), (10, state)):
                below = mid - low
                self.work[j, place + c] = (high - mid) - below
                self.work[j, place + 10 + c] = 0.75 * below

    def face(self, j):
        q, work, kept, r = self.q, self.work, self.kept, self.r
        mean = [q[c, rows_of(j + 2 * r), :] + q[c, rows_of(j + 3 * r), :] for c in self.order]
        inv = 1.0 / mean[0]
        vn, va, vb = mean[1] * inv, mean[2] * inv, mean[3] * inv
        kin = 0.5 * (vn * vn + va * va + vb * vb)
        c2 = GAMMA * (GAMMA - 1.0) * (mean[4] * inv - kin)
        ic = lax.rsqrt(c2)
        args = (vn, va, vb, kin, (0.5 * (GAMMA - 1.0)) * (ic * ic), 0.5 * ic)
        state = (vn, va, vb, kin, c2 * ic, (1.0 / (GAMMA - 1.0)) * c2 + kin)
        for k in range(6):
            kept[j, STATE + k] = state[k]
        places = [(k, 5, k - 1) for k in (1, 2, 3, 4)] + [(k, 10, k + 3) for k in (1, 2, 3, 4)]
        places += [(2, 15, 8), (4, 15, 9), (2, 20, 10), (4, 20, 11)]
        for cell, place, slot in places:
            u = project([work[j + cell * r, place + c] for c in range(5)], *args)
            for k in range(5):
                kept[j, FIELD * k + slot] = u[k]
        for c in range(5):
            near, far = work[j + 2 * r, c], work[j + 3 * r, c]
            kept[j, LINEAR + c] = 6.0 * (near + far) - work[j + 2 * r, 5 + c] - work[j + 3 * r, 5 + c]
            kept[j, LINEAR + 5 + c] = work[j + 3 * r, 10 + c] - work[j + 2 * r, 10 + c]

    def run(self, step, low, high, unroll=1):
        def body(t, _):
            step(t + low * self.r)
            return 0

        lax.fori_loop(0, (high - low) * self.r, body, 0, unroll=unroll)

    def inside(self):
        n = self.slots
        self.run(self.cell, 3, n + 3, 2)
        self.run(self.differ, 4, n + 2, 2)
        self.run(self.face, 3, n - 2, 2)

    def outside(self):
        n = self.slots
        for first, step, unroll in ((0, self.cell, 3), (1, self.differ, 3), (0, self.face, 3)):
            shift = n + 3 - 2 * first if step != self.face else n - 2
            self.run(step, first, first + 3, unroll)
            self.run(step, first + shift, first + shift + 3, unroll)


def face_flux(order, quarter, kept, j):
    n = []
    for k in range(5):
        a1, a2, a3, a4, b1, b2, b3, b4, ha, hb, sa, sb = (kept[j, FIELD * k + i] for i in range(FIELD))
        t2, t3 = quarter * b2, quarter * b3
        left = nonlinear(a1 + quarter * b1, a2 + t2, a3 + t3, ha + quarter * sa)
        right = nonlinear(a4 - quarter * b4, a3 - t3, a2 - t2, quarter * sb - hb)
        n.append(left + right)
    vn, va, vb, kin, sound, enthalpy = (kept[j, STATE + i] for i in range(6))
    d = sound * (n[4] - n[0])
    s15 = n[0] + n[4]
    s = s15 + n[3]
    out = [
        s,
        vn * s + d,
        va * s + n[1],
        vb * s + n[2],
        enthalpy * s15 + vn * d + va * n[1] + vb * n[2] + kin * n[3],
    ]
    flux = [None] * 5
    for c in range(5):
        flux[order[c]] = (kept[j, LINEAR + c] + quarter * kept[j, LINEAR + 5 + c]) + out[c]
    return flux


def sweep(direction, r, quarter, scale, kept, faces, place, low, high, unroll):
    def body(j, _):
        new = face_flux(ORDERS[direction], quarter, kept, j)
        old = [faces[j, c] for c in range(5)]
        for c in range(5):
            faces[j + r, c] = new[c]
        for c in range(5):
            place(j, c, scale * (old[c] - new[c]))
        return 0

    lax.fori_loop(low * r, high * r, body, 0, unroll=unroll)


def gather_kernel(
    sizes, stages, cells, shape, cons_hbm, kept_x, acc, factors, cons, kept_y, kept_z, faces, tz, qx, qy, qz, wx, wy, wz,
    xh, yh, zh, ysend, zsend, mine, theirs, halo_send, halo_recv, max_send, max_recv, load_sem,
):
    lx, ly, lz = shape
    rows = lx * ly
    groups = rows // LANES
    blocks = 8 // groups
    inner = lz // blocks
    load = pltpu.make_async_copy(cons_hbm, cons, load_sem)
    load.start()
    me = [lax.axis_index(axis) for axis in AXES]
    peers = []
    for axes in stages:
        group = []
        for shift in itertools.product(*[range(sizes[a]) for a in axes]):
            if any(shift):
                group.append({AXES[a]: lax.rem(me[a] + k, sizes[a]) for a, k in zip(axes, shift)})
        peers.append(group)
    barrier = pltpu.get_barrier_semaphore()
    count = 0
    for group in peers:
        for peer in group:
            pl.semaphore_signal(barrier, inc=1, device_id=peer, device_id_type=MESH)
            count += 1
    load.wait()

    best = [None] * 3
    for j in range(rows // 8):
        q = [cons[c, pl.ds(8 * j, 8), :] for c in range(5)]
        inv = 1.0 / q[0]
        vel = [q[d] * inv for d in (1, 2, 3)]
        kinetic = 0.5 * (vel[0] * vel[0] + vel[1] * vel[1] + vel[2] * vel[2])
        sound = jnp.sqrt((GAMMA * (GAMMA - 1.0)) * (q[4] * inv - kinetic))
        for d in range(3):
            value = jnp.abs(vel[d]) + sound
            best[d] = value if best[d] is None else jnp.maximum(best[d], value)
    lane = lax.broadcasted_iota(jnp.int32, (1, LANES), 1)
    local = [jnp.max(jnp.max(v, axis=0, keepdims=True), axis=1, keepdims=True) for v in best]
    mine[0] = jnp.where(lane == 0, local[0], jnp.where(lane == 1, local[1], local[2]))

    for c in range(5):
        for k in range(3):
            ysend[0, c, pl.ds(k * lx, lx), :] = cons[c, pl.ds(ly - 3 + k, lx, stride=ly), :]
            ysend[1, c, pl.ds(k * lx, lx), :] = cons[c, pl.ds(k, lx, stride=ly), :]
    for c in range(5):
        for g in range(groups):
            turned = jnp.transpose(cons[c, pl.ds(g * LANES, LANES), :])
            for b in range(blocks):
                qz[c, pl.ds(24 + b * groups + g, inner, stride=8), :] = turned[b * inner:(b + 1) * inner]
            for k in range(3):
                zsend[0, pl.ds((3 * c + k) * groups + g, 1), :] = turned[lz - 3 + k:lz - 2 + k]
                zsend[1, pl.ds((3 * c + k) * groups + g, 1), :] = turned[k:k + 1]
    x_edge, y_edge = 3 * ly, 3 * lx
    for c in range(5):
        for y in range(ly):
            qy[c, pl.ds(y_edge + y * lx, lx), :] = cons[c, pl.ds(y, lx, stride=ly), :]
    qx[:, pl.ds(x_edge, rows), :] = cons[...]

    along = [
        Sweep(0, lx, ly // 8, qx, wx, kept_x),
        Sweep(1, ly, lx // 8, qy, wy, kept_y),
        Sweep(2, inner, 1, qz, wz, kept_z),
    ]
    for axis in (0,):
        along[axis].inside()

    def halo(slot, src, dst, axis, up):
        size = sizes[axis]
        target = lax.rem(me[axis] + (1 if up else size - 1), size)
        return pltpu.make_async_remote_copy(
            src_ref=src, dst_ref=dst, send_sem=halo_send.at[slot], recv_sem=halo_recv.at[slot],
            device_id={AXES[axis]: target}, device_id_type=MESH,
        )

    def spread(stage):
        copies = []
        first = sum(len(group) for group in peers[:stage])
        for k, peer in enumerate(peers[stage]):
            slot = first + k
            copy = pltpu.make_async_remote_copy(
                src_ref=mine.at[stage], dst_ref=theirs.at[slot],
                send_sem=max_send.at[slot], recv_sem=max_recv.at[slot],
                device_id=peer, device_id_type=MESH,
            )
            copy.start()
            copies.append((slot, copy))
        return copies

    def gather(stage, copies):
        value = mine[stage]
        for slot, copy in copies:
            copy.wait_recv()
            value = jnp.maximum(value, theirs[slot])
        return value

    pl.semaphore_wait(barrier, count)
    sent = [spread(0)]
    halos = [
        [
            halo(0, cons.at[:, pl.ds(rows - x_edge, x_edge), :], xh.at[0], 0, True),
            halo(1, cons.at[:, pl.ds(0, x_edge), :], xh.at[1], 0, False),
        ],
        [halo(2, ysend.at[0], yh.at[0], 1, True), halo(3, ysend.at[1], yh.at[1], 1, False)],
        [halo(4, zsend.at[0], zh.at[0], 2, True), halo(5, zsend.at[1], zh.at[1], 2, False)],
    ]
    for axis in (2, 1, 0):
        for copy in halos[axis]:
            copy.start()

    def fill_y():
        for copy in halos[1]:
            copy.wait()
        qy[:, pl.ds(0, y_edge), :] = yh[0]
        qy[:, pl.ds(y_edge + rows, y_edge), :] = yh[1]
        along[1].outside()

    def fill_z():
        for copy in halos[2]:
            copy.wait()
        size = inner * 8
        for c in range(5):
            for k in range(3):
                low, high = 8 * k, 24 + size + 8 * k
                qz[c, low:low + groups, :] = zh[0, pl.ds((3 * c + k) * groups, groups), :]
                qz[c, low + groups:low + 8, :] = qz[c, size + 8 * k:size + 8 + 8 * k - groups, :]
                qz[c, high:high + 8 - groups, :] = qz[c, 24 + 8 * k + groups:32 + 8 * k, :]
                qz[c, high + 8 - groups:high + 8, :] = zh[1, pl.ds((3 * c + k) * groups, groups), :]
        along[2].outside()

    def fill_x():
        for copy in halos[0]:
            copy.wait()
        qx[:, pl.ds(0, x_edge), :] = xh[0]
        qx[:, pl.ds(x_edge + rows, x_edge), :] = xh[1]
        along[0].outside()

    for axis in (2, 1):
        along[axis].inside()
    fill_y()
    fill_z()
    for stage in range(1, len(stages)):
        mine[stage] = gather(stage - 1, sent[-1])
        sent.append(spread(stage))
    top = gather(len(stages) - 1, sent[-1])
    for copies in sent:
        for _, copy in copies:
            copy.wait_send()
    speed = [jnp.broadcast_to(top[:, d:d + 1], (8, LANES)) for d in range(3)]
    step = COURANT / (speed[0] * cells[0] + speed[1] * cells[1] + speed[2] * cells[2])
    factors[0] = 0.25 * speed[0]
    factors[1] = step * (cells[0] / 3.0)

    ry = lx // 8

    def place_y(j, c, value):
        y = jnp.maximum(j // ry - 1, 0)
        acc[c, pl.ds(8 * ly * (j % ry) + y, 8, stride=ly), :] = value

    def place_z(j, c, value):
        tz[c, rows_of(jnp.maximum(j - 1, 0)), :] = value

    for axis, r, slots, place in ((1, ry, ly, place_y), (2, 1, inner, place_z)):
        scale = step * (cells[axis] / 3.0)
        sweep(axis, r, 0.25 * speed[axis], scale, along[axis].kept, faces, place, 0, slots + 1, (2, 3)[axis - 1])
    for c in range(5):
        for g in range(groups):
            parts = [tz[c, pl.ds(b * groups + g, inner, stride=8), :] for b in range(blocks)]
            turned = jnp.transpose(jnp.concatenate(parts, axis=0))
            here = pl.ds(g * LANES, LANES)
            acc[c, here, :] = (cons[c, here, :] + acc[c, here, :]) + turned
    fill_x()


def combine_kernel(shape, kept, acc, factors, out_hbm, out, faces, store_sem):
    lx, ly, lz = shape
    rx = ly // 8
    quarter, scale = factors[0], factors[1]

    def place(j, c, value):
        x = jnp.maximum(j // rx - 1, 0)
        here = rows_of(x * rx + j % rx)
        out[c, here, :] = acc[c, here, :] + value

    stores = []
    chunk = lx // 4
    for m in range(4):
        sweep(0, rx, quarter, scale, kept, faces, place, 0 if m == 0 else m * chunk + 1, (m + 1) * chunk + 1, 2)
        part = pl.ds(m * chunk * ly, chunk * ly)
        stores.append(pltpu.make_async_copy(out.at[:, part, :], out_hbm.at[:, part, :], store_sem.at[m]))
        stores[-1].start()
    for store in stores:
        store.wait()


def solution(mesh):
    sizes = [mesh.shape[axis] for axis in AXES]
    stages = [(0, 1, 2)] if sizes[0] * sizes[1] * sizes[2] <= 64 else [(0,), (2,), (1,)]

    def per_device(conserved):
        _, lx, ly, lz = conserved.shape
        shape = (lx, ly, lz)
        cells = [float(n * s) for n, s in zip(shape, sizes)]
        rows = lx * ly
        groups = rows // LANES
        inner = lz * groups // 8
        assert lz == LANES and rows % LANES == 0 and 8 % groups == 0 and lx % 8 == 0 and ly % 8 == 0
        total = 0
        for axes in stages:
            size = 1
            for a in axes:
                size *= sizes[a]
            total += size - 1

        def vmem(*dims):
            return pltpu.VMEM(dims, jnp.float32)

        def faces(count):
            return vmem(count, KEPT, 8, LANES)

        pads = [(lx + 6) * ly // 8, (ly + 6) * lx // 8, inner + 6]
        kept = [faces((lx + 1) * ly // 8), faces((ly + 1) * lx // 8), faces(inner + 1)]
        flux = vmem(max((lx + 2) * ly // 8, (ly + 2) * lx // 8, inner + 2), 5, 8, LANES)
        block = vmem(5, rows, lz)
        whole = pl.BlockSpec(memory_space=pltpu.VMEM)
        kept_x, acc, factors = pl.pallas_call(
            functools.partial(gather_kernel, sizes, stages, cells, shape),
            name="gather",
            out_shape=[kept[0], block, vmem(2, 8, LANES)],
            in_specs=[pl.BlockSpec(memory_space=pltpu.HBM)],
            out_specs=[whole] * 3,
            scratch_shapes=[block, kept[1], kept[2], flux, vmem(5, 8 * inner, LANES)]
            + [vmem(5, 8 * n, LANES) for n in pads] + [vmem(n, 25, 8, LANES) for n in pads] + [
                vmem(2, 5, 3 * ly, lz),
                vmem(2, 5, 3 * lx, lz),
                vmem(2, 15 * groups, LANES),
                vmem(2, 5, 3 * lx, lz),
                vmem(2, 15 * groups, LANES),
                vmem(len(stages), 1, LANES),
                vmem(total, 1, LANES),
                pltpu.SemaphoreType.DMA((6,)),
                pltpu.SemaphoreType.DMA((6,)),
                pltpu.SemaphoreType.DMA((total,)),
                pltpu.SemaphoreType.DMA((total,)),
                pltpu.SemaphoreType.DMA,
            ],
            compiler_params=pltpu.CompilerParams(
                collective_id=0, has_side_effects=True, vmem_limit_bytes=44 * 2**20
            ),
        )(pltpu.with_memory_space_constraint(conserved.reshape(5, rows, lz), pltpu.HBM))
        out = pl.pallas_call(
            functools.partial(combine_kernel, shape),
            name="combine",
            out_shape=jax.ShapeDtypeStruct((5, rows, lz), jnp.float32),
            in_specs=[whole] * 3,
            out_specs=pl.BlockSpec(memory_space=pl.ANY),
            scratch_shapes=[block, flux, pltpu.SemaphoreType.DMA((4,))],
            compiler_params=pltpu.CompilerParams(vmem_limit_bytes=16 * 2**20),
        )(kept_x, acc, factors)
        return out.reshape(conserved.shape)

    return jax.shard_map(
        per_device,
        mesh=mesh,
        in_specs=(P(None, "gx", "gy", "gz"),),
        out_specs=P(None, "gx", "gy", "gz"),
        check_vma=False,
    )
```

```python
import functools

import jax
import jax.numpy as jnp
from jax import lax
from jax.experimental import pallas as pl
from jax.experimental.pallas import tpu as pltpu
from jax.sharding import PartitionSpec as P

GAMMA = 1.4
EPS = 1e-06 * (3.0 / 16.0)
COURANT = 0.4
MESH = pl.DeviceIdType.MESH
AXES = ("gx", "gy", "gz")
ORDERS = ([0, 1, 2, 3, 4], [0, 2, 1, 3, 4], [0, 3, 1, 2, 4])
LANES = 128
FIELD = 12
STATE = 5 * FIELD
LINEAR = STATE + 6
KEPT = LINEAR + 10


def project(u, vn, va, vb, kin, b1h, ich):
    a = u[4] + kin * u[0] - vn * u[1] - va * u[2] - vb * u[3]
    a = b1h * a
    b = (vn * u[0] - u[1]) * ich
    return [a + b, u[2] - va * u[0], u[3] - vb * u[0], u[0] - (a + a), a - b]


def nonlinear(e1, e2, e3, h):
    c = ((4.0 / 3.0) * h) * h + EPS
    g = h + 0.75 * e2
    q0 = 1.0 / (e1 * (e1 + h) + c)
    q1 = 1.0 / (e2 * (e2 + h) + c)
    q2 = 1.0 / (e3 * (e3 - g) + (((4.0 / 3.0) * g) * g + EPS))
    w0 = q0 * q0
    w2 = 3.0 * (q2 * q2)
    n0 = e1 - e2
    return (w0 * (n0 + n0) + w2 * (e2 - e3)) / (w0 + w2 + 6.0 * (q1 * q1))


def rows_of(j):
    return pl.ds(pl.multiple_of(8 * j, 8), 8)


class Sweep:
    def __init__(self, direction, slots, lane_rows, q, work, kept):
        self.order = ORDERS[direction]
        self.slots, self.r = slots, lane_rows
        self.q, self.work, self.kept = q, work, kept

    def cell(self, j):
        s = [self.q[c, rows_of(j), :] for c in self.order]
        inv = 1.0 / s[0]
        vq = s[1] * (0.25 * inv)
        pq = 0.25 * (GAMMA - 1.0) * (s[4] - (0.5 * inv) * (s[1] * s[1] + s[2] * s[2] + s[3] * s[3]))
        f = [0.25 * s[1], s[1] * vq + pq, s[2] * vq, s[3] * vq, s[4] * vq + 4.0 * (pq * vq)]
        for c in range(5):
            self.work[j, c] = f[c]

    def differ(self, j):
        r = self.r
        for c in range(5):
            flux = [self.work[j + k * r, c] for k in (-1, 0, 1)]
            state = [self.q[self.order[c], rows_of(j + k * r), :] for k in (-1, 0, 1)]
            for place, (low, mid, high) in ((5, flux), (10, state)):
                below = mid - low
                self.work[j, place + c] = (high - mid) - below
                self.work[j, place + 10 + c] = 0.75 * below

    def face(self, j):
        q, work, kept, r = self.q, self.work, self.kept, self.r
        mean = [q[c, rows_of(j + 2 * r), :] + q[c, rows_of(j + 3 * r), :] for c in self.order]
        inv = 1.0 / mean[0]
        vn, va, vb = mean[1] * inv, mean[2] * inv, mean[3] * inv
        kin = 0.5 * (vn * vn + va * va + vb * vb)
        c2 = GAMMA * (GAMMA - 1.0) * (mean[4] * inv - kin)
        ic = lax.rsqrt(c2)
        args = (vn, va, vb, kin, (0.5 * (GAMMA - 1.0)) * (ic * ic), 0.5 * ic)
        state = (vn, va, vb, kin, c2 * ic, (1.0 / (GAMMA - 1.0)) * c2 + kin)
        for k in range(6):
            kept[j, STATE + k] = state[k]
        places = [(k, 5, k - 1) for k in (1, 2, 3, 4)] + [(k, 10, k + 3) for k in (1, 2, 3, 4)]
        places += [(2, 15, 8), (4, 15, 9), (2, 20, 10), (4, 20, 11)]
        for cell, place, slot in places:
            u = project([work[j + cell * r, place + c] for c in range(5)], *args)
            for k in range(5):
                kept[j, FIELD * k + slot] = u[k]
        for c in range(5):
            near, far = work[j + 2 * r, c], work[j + 3 * r, c]
            kept[j, LINEAR + c] = 6.0 * (near + far) - work[j + 2 * r, 5 + c] - work[j + 3 * r, 5 + c]
            kept[j, LINEAR + 5 + c] = work[j + 3 * r, 10 + c] - work[j + 2 * r, 10 + c]

    def run(self, step, low, high, unroll=1):
        def body(t, _):
            step(t + low * self.r)
            return 0

        lax.fori_loop(0, (high - low) * self.r, body, 0, unroll=unroll)

    def cells_inside(self):
        n = self.slots
        self.run(self.cell, 3, n + 3, 4)
        self.run(self.differ, 4, n + 2, 4 if self.r > 1 else 6)

    def faces_inside(self):
        self.run(self.face, 3, self.slots - 2, 4 - self.r)

    def inside(self):
        self.cells_inside()
        self.faces_inside()

    def outside(self):
        n = self.slots
        for first, step, unroll in ((0, self.cell, 3), (1, self.differ, 3), (0, self.face, 3)):
            shift = n + 3 - 2 * first if step != self.face else n - 2
            self.run(step, first, first + 3, unroll)
            self.run(step, first + shift, first + shift + 3, unroll)


def face_flux(order, quarter, kept, j):
    n = []
    for k in range(5):
        a1, a2, a3, a4, b1, b2, b3, b4, ha, hb, sa, sb = (kept[j, FIELD * k + i] for i in range(FIELD))
        t2, t3 = quarter * b2, quarter * b3
        left = nonlinear(a1 + quarter * b1, a2 + t2, a3 + t3, ha + quarter * sa)
        right = nonlinear(a4 - quarter * b4, a3 - t3, a2 - t2, quarter * sb - hb)
        n.append(left + right)
    vn, va, vb, kin, sound, enthalpy = (kept[j, STATE + i] for i in range(6))
    d = sound * (n[4] - n[0])
    s15 = n[0] + n[4]
    s = s15 + n[3]
    out = [
        s,
        vn * s + d,
        va * s + n[1],
        vb * s + n[2],
        enthalpy * s15 + vn * d + va * n[1] + vb * n[2] + kin * n[3],
    ]
    flux = [None] * 5
    for c in range(5):
        flux[order[c]] = (kept[j, LINEAR + c] + quarter * kept[j, LINEAR + 5 + c]) + out[c]
    return flux


def sweep(direction, r, quarter, scale, kept, faces, place, low, high, unroll):
    def body(j, _):
        new = face_flux(ORDERS[direction], quarter, kept, j)
        old = [faces[j, c] for c in range(5)]
        for c in range(5):
            faces[j + r, c] = new[c]
        for c in range(5):
            change = old[c] - new[c]
            place(j, c, change if scale is None else scale * change)
        return 0

    lax.fori_loop(low * r, high * r, body, 0, unroll=unroll)


def gather_kernel(
    sizes, cells, shape, cons_hbm, kept_x, acc, factors, kept_y, kept_z, faces, tz, qx, qy, qz, wx, wy, wz,
    zh, zsend, top, mine, theirs, halo_send, halo_recv, max_send, max_recv, load_sem, turn_sem,
):
    lx, ly, lz = shape
    rows = lx * ly
    groups = rows // LANES
    blocks = 8 // groups
    inner = lz // blocks
    x_edge, y_edge = 3 * ly, 3 * lx
    cons = qx.at[:, pl.ds(x_edge, rows), :]
    turned_y = qy.at[:, pl.ds(y_edge, rows), :]
    load = pltpu.make_async_copy(cons_hbm.reshape(5, rows, lz), cons, load_sem)
    load.start()
    for y in range(ly):
        pltpu.make_async_copy(cons_hbm.at[:, :, y, :], qy.at[:, pl.ds(y_edge + y * lx, lx), :], turn_sem).start()
    me = [lax.axis_index(axis) for axis in AXES]
    count = sizes[0] * sizes[1] * sizes[2]
    plane = sizes[0] * sizes[2]
    place = (me[0] * sizes[1] + me[1]) * sizes[2] + me[2]
    is_root = me[0] + me[2] == 0
    roots = [{"gx": 0, "gy": r, "gz": 0} for r in range(sizes[1])]

    def beside(axis, up):
        return {AXES[axis]: lax.rem(me[axis] + (1 if up else sizes[axis] - 1), sizes[axis])}

    barrier = pltpu.get_barrier_semaphore()

    def greet(peer):
        pl.semaphore_signal(barrier, inc=1, device_id=peer, device_id_type=MESH)

    for axis in range(3):
        for up in (True, False):
            greet(beside(axis, up))

    @pl.when(is_root)
    def _():
        def tell(t, _):
            other = lax.rem(place + t, count)
            rest = other // sizes[2]
            greet({"gx": rest // sizes[1], "gy": rest % sizes[1], "gz": other % sizes[2]})
            return 0

        lax.fori_loop(1, count, tell, 0)

    load.wait()

    best = [None] * 3
    for j in range(rows // 8):
        q = [qx[c, pl.ds(x_edge + 8 * j, 8), :] for c in range(5)]
        inv = 1.0 / q[0]
        vel = [q[d] * inv for d in (1, 2, 3)]
        kinetic = 0.5 * (vel[0] * vel[0] + vel[1] * vel[1] + vel[2] * vel[2])
        sound = jnp.sqrt((GAMMA * (GAMMA - 1.0)) * (q[4] * inv - kinetic))
        for d in range(3):
            value = jnp.abs(vel[d]) + sound
            best[d] = value if best[d] is None else jnp.maximum(best[d], value)
    lane = lax.broadcasted_iota(jnp.int32, (1, LANES), 1)
    local = [jnp.max(jnp.max(v, axis=0, keepdims=True), axis=1, keepdims=True) for v in best]
    mine[...] = jnp.where(lane == 0, local[0], jnp.where(lane == 1, local[1], local[2]))

    for c in range(5):
        for g in range(groups):
            turned = jnp.transpose(qx[c, pl.ds(x_edge + g * LANES, LANES), :])
            for b in range(blocks):
                qz[c, pl.ds(24 + b * groups + g, inner, stride=8), :] = turned[b * inner:(b + 1) * inner]
            for k in range(3):
                zsend[0, pl.ds((3 * c + k) * groups + g, 1), :] = turned[lz - 3 + k:lz - 2 + k]
                zsend[1, pl.ds((3 * c + k) * groups + g, 1), :] = turned[k:k + 1]
    along = [
        Sweep(0, lx, ly // 8, qx, wx, kept_x),
        Sweep(1, ly, lx // 8, qy, wy, kept_y),
        Sweep(2, inner, 1, qz, wz, kept_z),
    ]
    pltpu.make_async_copy(turned_y, turned_y, turn_sem).wait()

    @pl.when(is_root)
    def _():
        for axis in (0,):
            along[axis].inside()

    def halo(slot, src, dst, axis, up):
        return pltpu.make_async_remote_copy(
            src_ref=src, dst_ref=dst, send_sem=halo_send.at[slot], recv_sem=halo_recv.at[slot],
            device_id=beside(axis, up), device_id_type=MESH,
        )

    pl.semaphore_wait(barrier, 6 + sizes[1] - jnp.where(is_root, 1, 0))
    reports = []
    for r, root in enumerate(roots):
        slot = lax.rem(place - r * sizes[2] + count - 1, count)
        report = pltpu.make_async_remote_copy(
            src_ref=mine, dst_ref=theirs.at[slot], send_sem=max_send.at[r], recv_sem=max_recv.at[0],
            device_id=root, device_id_type=MESH,
        )
        pl.when(place != r * sizes[2])(report.start)
        reports.append(report)
    halos = [
        [
            halo(0, qx.at[:, pl.ds(rows, x_edge), :], qx.at[:, pl.ds(0, x_edge), :], 0, True),
            halo(1, qx.at[:, pl.ds(x_edge, x_edge), :], qx.at[:, pl.ds(x_edge + rows, x_edge), :], 0, False),
        ],
        [
            halo(2, qy.at[:, pl.ds(rows, y_edge), :], qy.at[:, pl.ds(0, y_edge), :], 1, True),
            halo(3, qy.at[:, pl.ds(y_edge, y_edge), :], qy.at[:, pl.ds(y_edge + rows, y_edge), :], 1, False),
        ],
        [halo(4, zsend.at[0], zh.at[0], 2, True), halo(5, zsend.at[1], zh.at[1], 2, False)],
    ]
    for axis in (2, 1, 0):
        for copy in halos[axis]:
            copy.start()

    def fill_y():
        for copy in halos[1]:
            copy.wait()
        along[1].outside()

    def fill_z():
        for copy in halos[2]:
            copy.wait()
        size = inner * 8
        for c in range(5):
            for k in range(3):
                low, high = 8 * k, 24 + size + 8 * k
                qz[c, low:low + groups, :] = zh[0, pl.ds((3 * c + k) * groups, groups), :]
                qz[c, low + groups:low + 8, :] = qz[c, size + 8 * k:size + 8 + 8 * k - groups, :]
                qz[c, high:high + 8 - groups, :] = qz[c, 24 + 8 * k + groups:32 + 8 * k, :]
                qz[c, high + 8 - groups:high + 8, :] = zh[1, pl.ds((3 * c + k) * groups, groups), :]
        along[2].outside()

    def fill_x():
        for copy in halos[0]:
            copy.wait()
        along[0].outside()

    def answer(peer):
        return pltpu.make_async_remote_copy(
            src_ref=top, dst_ref=top, send_sem=max_send.at[sizes[1]], recv_sem=max_recv.at[1],
            device_id=peer, device_id_type=MESH,
        )

    def bytes_of(refs, send, receive):
        return pltpu.make_async_remote_copy(
            src_ref=refs, dst_ref=refs, send_sem=max_send.at[send], recv_sem=max_recv.at[receive],
            device_id=beside(1, True), device_id_type=MESH,
        )

    @pl.when(is_root)
    def _():
        for axis in (2, 1):
            along[axis].inside()
        fill_y()
        bytes_of(theirs, 0, 0).wait_recv()
        top[...] = jnp.maximum(mine[...], jnp.max(theirs[...], axis=0))

        def tell(t, _):
            answer({"gx": t // sizes[2], "gy": me[1], "gz": t % sizes[2]}).start()
            return 0

        lax.fori_loop(1, plane, tell, 0)

    @pl.when(jnp.logical_not(is_root))
    def _():
        for axis in (1, 2, 0):
            along[axis].inside()
        fill_y()
        fill_z()
        answer(beside(1, True)).wait_recv()

    for r, report in enumerate(reports):
        pl.when(place != r * sizes[2])(report.wait_send)
    speed = [jnp.broadcast_to(top[0:1, d:d + 1], (8, LANES)) for d in range(3)]
    step = COURANT / (speed[0] * cells[0] + speed[1] * cells[1] + speed[2] * cells[2])
    factors[0] = 0.25 * speed[0]
    factors[1] = step * (cells[0] / 3.0)

    ry = lx // 8

    def place_y(j, c, value):
        y = jnp.maximum(j // ry - 1, 0)
        acc[c, pl.ds(8 * ly * (j % ry) + y, 8, stride=ly), :] = value

    def place_z(j, c, value):
        tz[c, rows_of(jnp.maximum(j - 1, 0)), :] = value

    def combine(axis, r, slots, put, unroll):
        sweep(axis, r, 0.25 * speed[axis], None, along[axis].kept, faces, put, 0, slots + 1, unroll)

    combine(1, ry, ly, place_y, 2)
    pl.when(is_root)(fill_z)
    combine(2, 1, inner, place_z, 3)
    scale = [(step * (cells[d] / 3.0))[:1] for d in range(3)]
    for c in range(5):
        for g in range(groups):
            parts = [tz[c, pl.ds(b * groups + g, inner, stride=8), :] for b in range(blocks)]
            turned = jnp.transpose(jnp.concatenate(parts, axis=0))
            here = pl.ds(g * LANES, LANES)
            held = qx[c, pl.ds(x_edge + g * LANES, LANES), :] + scale[1] * acc[c, here, :]
            acc[c, here, :] = held + scale[2] * turned
    fill_x()

    @pl.when(is_root)
    def _():
        bytes_of(theirs.at[pl.ds(0, plane - 1)], sizes[1], 1).wait_send()


def combine_kernel(shape, kept, acc, factors, out_hbm, out, faces, store_sem):
    lx, ly, lz = shape
    rx = ly // 8
    quarter, scale = factors[0], factors[1]

    def place(j, c, value):
        x = jnp.maximum(j // rx - 1, 0)
        here = rows_of(x * rx + j % rx)
        out[c, here, :] = acc[c, here, :] + value

    stores = []
    chunk = lx // 4
    for m in range(4):
        sweep(0, rx, quarter, scale, kept, faces, place, 0 if m == 0 else m * chunk + 1, (m + 1) * chunk + 1, 2)
        part = pl.ds(m * chunk * ly, chunk * ly)
        stores.append(pltpu.make_async_copy(out.at[:, part, :], out_hbm.at[:, part, :], store_sem.at[m]))
        stores[-1].start()
    for store in stores:
        store.wait()


def solution(mesh):
    sizes = [mesh.shape[axis] for axis in AXES]
    count = sizes[0] * sizes[1] * sizes[2]

    def per_device(conserved):
        _, lx, ly, lz = conserved.shape
        shape = (lx, ly, lz)
        cells = [float(n * s) for n, s in zip(shape, sizes)]
        rows = lx * ly
        groups = rows // LANES
        inner = lz * groups // 8
        assert lz == LANES and rows % LANES == 0 and 8 % groups == 0 and lx % 8 == 0 and ly % 8 == 0
        def vmem(*dims):
            return pltpu.VMEM(dims, jnp.float32)

        def faces(count):
            return vmem(count, KEPT, 8, LANES)

        pads = [(lx + 6) * ly // 8, (ly + 6) * lx // 8, inner + 6]
        kept = [faces((lx + 1) * ly // 8), faces((ly + 1) * lx // 8), faces(inner + 1)]
        flux = vmem(max((lx + 2) * ly // 8, (ly + 2) * lx // 8, inner + 2), 5, 8, LANES)
        block = vmem(5, rows, lz)
        whole = pl.BlockSpec(memory_space=pltpu.VMEM)
        kept_x, acc, factors = pl.pallas_call(
            functools.partial(gather_kernel, sizes, cells, shape),
            name="gather",
            out_shape=[kept[0], block, vmem(2, 8, LANES)],
            in_specs=[pl.BlockSpec(memory_space=pltpu.HBM)],
            out_specs=[whole] * 3,
            scratch_shapes=[kept[1], kept[2], flux, vmem(5, 8 * inner, LANES)]
            + [vmem(5, 8 * n, LANES) for n in pads] + [vmem(n, 25, 8, LANES) for n in pads] + [
                vmem(2, 15 * groups, LANES),
                vmem(2, 15 * groups, LANES),
                vmem(1, LANES),
                vmem(1, LANES),
                vmem(count - 1, 1, LANES),
                pltpu.SemaphoreType.DMA((6,)),
                pltpu.SemaphoreType.DMA((6,)),
                pltpu.SemaphoreType.DMA((sizes[1] + 1,)),
                pltpu.SemaphoreType.DMA((2,)),
                pltpu.SemaphoreType.DMA,
                pltpu.SemaphoreType.DMA,
            ],
            compiler_params=pltpu.CompilerParams(
                collective_id=0, has_side_effects=True, vmem_limit_bytes=44 * 2**20
            ),
        )(pltpu.with_memory_space_constraint(conserved, pltpu.HBM))
        out = pl.pallas_call(
            functools.partial(combine_kernel, shape),
            name="combine",
            out_shape=jax.ShapeDtypeStruct((5, rows, lz), jnp.float32),
            in_specs=[whole] * 3,
            out_specs=pl.BlockSpec(memory_space=pl.ANY),
            scratch_shapes=[block, flux, pltpu.SemaphoreType.DMA((4,))],
            compiler_params=pltpu.CompilerParams(vmem_limit_bytes=16 * 2**20),
        )(kept_x, acc, factors)
        return out.reshape(conserved.shape)

    return jax.shard_map(
        per_device,
        mesh=mesh,
        in_specs=(P(None, "gx", "gy", "gz"),),
        out_specs=P(None, "gx", "gy", "gz"),
        check_vma=False,
    )
```

```python
import functools

import jax
import jax.numpy as jnp
from jax import lax
from jax.experimental import pallas as pl
from jax.experimental.pallas import tpu as pltpu
from jax.sharding import PartitionSpec as P

GAMMA = 1.4
EPS = 1e-06 * (3.0 / 16.0)
COURANT = 0.4
MESH = pl.DeviceIdType.MESH
AXES = ("gx", "gy", "gz")
ORDERS = ([0, 1, 2, 3, 4], [0, 2, 1, 3, 4], [0, 3, 1, 2, 4])
LANES = 128
FIELD = 12
STATE = 5 * FIELD
LINEAR = STATE + 6
KEPT = LINEAR + 10


def project(u, vn, va, vb, kin, b1h, ich):
    a = u[4] + kin * u[0] - vn * u[1] - va * u[2] - vb * u[3]
    a = b1h * a
    b = (vn * u[0] - u[1]) * ich
    return [a + b, u[2] - va * u[0], u[3] - vb * u[0], u[0] - (a + a), a - b]


def nonlinear(e1, e2, e3, h):
    c = ((4.0 / 3.0) * h) * h + EPS
    g = h + 0.75 * e2
    q0 = 1.0 / (e1 * (e1 + h) + c)
    q1 = 1.0 / (e2 * (e2 + h) + c)
    q2 = 1.0 / (e3 * (e3 - g) + (((4.0 / 3.0) * g) * g + EPS))
    w0 = q0 * q0
    w2 = 3.0 * (q2 * q2)
    n0 = e1 - e2
    return (w0 * (n0 + n0) + w2 * (e2 - e3)) / (w0 + w2 + 6.0 * (q1 * q1))


def rows_of(j):
    return pl.ds(pl.multiple_of(8 * j, 8), 8)


class Sweep:
    def __init__(self, direction, slots, lane_rows, q, work, kept):
        self.order = ORDERS[direction]
        self.slots, self.r = slots, lane_rows
        self.q, self.work, self.kept = q, work, kept

    def cell(self, j):
        s = [self.q[c, rows_of(j), :] for c in self.order]
        inv = 1.0 / s[0]
        vq = s[1] * (0.25 * inv)
        pq = 0.25 * (GAMMA - 1.0) * (s[4] - (0.5 * inv) * (s[1] * s[1] + s[2] * s[2] + s[3] * s[3]))
        f = [0.25 * s[1], s[1] * vq + pq, s[2] * vq, s[3] * vq, s[4] * vq + 4.0 * (pq * vq)]
        for c in range(5):
            self.work[j, c] = f[c]

    def differ(self, j):
        r = self.r
        for c in range(5):
            flux = [self.work[j + k * r, c] for k in (-1, 0, 1)]
            state = [self.q[self.order[c], rows_of(j + k * r), :] for k in (-1, 0, 1)]
            for place, (low, mid, high) in ((5, flux), (10, state)):
                below = mid - low
                self.work[j, place + c] = (high - mid) - below
                self.work[j, place + 10 + c] = 0.75 * below

    def face(self, j):
        q, work, kept, r = self.q, self.work, self.kept, self.r
        mean = [q[c, rows_of(j + 2 * r), :] + q[c, rows_of(j + 3 * r), :] for c in self.order]
        inv = 1.0 / mean[0]
        vn, va, vb = mean[1] * inv, mean[2] * inv, mean[3] * inv
        kin = 0.5 * (vn * vn + va * va + vb * vb)
        c2 = GAMMA * (GAMMA - 1.0) * (mean[4] * inv - kin)
        ic = lax.rsqrt(c2)
        args = (vn, va, vb, kin, (0.5 * (GAMMA - 1.0)) * (ic * ic), 0.5 * ic)
        state = (vn, va, vb, kin, c2 * ic, (1.0 / (GAMMA - 1.0)) * c2 + kin)
        for k in range(6):
            kept[j, STATE + k] = state[k]
        places = [(k, 5, k - 1) for k in (1, 2, 3, 4)] + [(k, 10, k + 3) for k in (1, 2, 3, 4)]
        places += [(2, 15, 8), (4, 15, 9), (2, 20, 10), (4, 20, 11)]
        for cell, place, slot in places:
            u = project([work[j + cell * r, place + c] for c in range(5)], *args)
            for k in range(5):
                kept[j, FIELD * k + slot] = u[k]
        for c in range(5):
            near, far = work[j + 2 * r, c], work[j + 3 * r, c]
            kept[j, LINEAR + c] = 6.0 * (near + far) - work[j + 2 * r, 5 + c] - work[j + 3 * r, 5 + c]
            kept[j, LINEAR + 5 + c] = work[j + 3 * r, 10 + c] - work[j + 2 * r, 10 + c]

    def run(self, step, low, high, unroll=1):
        def body(t, _):
            step(t + low * self.r)
            return 0

        lax.fori_loop(0, (high - low) * self.r, body, 0, unroll=unroll)

    def cells_inside(self):
        n = self.slots
        self.run(self.cell, 3, n + 3, 4)
        self.run(self.differ, 4, n + 2, 4 if self.r > 1 else 6)

    def faces_inside(self):
        self.run(self.face, 3, self.slots - 2, 4 - self.r)

    def inside(self):
        self.cells_inside()
        self.faces_inside()

    def outside(self):
        n = self.slots
        for first, step, unroll in ((0, self.cell, 3), (1, self.differ, 3), (0, self.face, 3)):
            shift = n + 3 - 2 * first if step != self.face else n - 2
            self.run(step, first, first + 3, unroll)
            self.run(step, first + shift, first + shift + 3, unroll)


def face_flux(order, quarter, kept, j):
    n = []
    for k in range(5):
        a1, a2, a3, a4, b1, b2, b3, b4, ha, hb, sa, sb = (kept[j, FIELD * k + i] for i in range(FIELD))
        t2, t3 = quarter * b2, quarter * b3
        left = nonlinear(a1 + quarter * b1, a2 + t2, a3 + t3, ha + quarter * sa)
        right = nonlinear(a4 - quarter * b4, a3 - t3, a2 - t2, quarter * sb - hb)
        n.append(left + right)
    vn, va, vb, kin, sound, enthalpy = (kept[j, STATE + i] for i in range(6))
    d = sound * (n[4] - n[0])
    s15 = n[0] + n[4]
    s = s15 + n[3]
    out = [
        s,
        vn * s + d,
        va * s + n[1],
        vb * s + n[2],
        enthalpy * s15 + vn * d + va * n[1] + vb * n[2] + kin * n[3],
    ]
    flux = [None] * 5
    for c in range(5):
        flux[order[c]] = (kept[j, LINEAR + c] + quarter * kept[j, LINEAR + 5 + c]) + out[c]
    return flux


def sweep(direction, r, quarter, scale, kept, faces, place, low, high, unroll):
    def body(j, _):
        new = face_flux(ORDERS[direction], quarter, kept, j)
        old = [faces[j, c] for c in range(5)]
        for c in range(5):
            faces[j + r, c] = new[c]
        for c in range(5):
            change = old[c] - new[c]
            place(j, c, change if scale is None else scale * change)
        return 0

    lax.fori_loop(low * r, high * r, body, 0, unroll=unroll)


def gather_kernel(
    sizes, cells, shape, cons_hbm, kept_x, acc, factors, kept_y, kept_z, faces, tz, qx, qy, qz, wx, wy, wz,
    zh, zsend, top, mine, theirs, halo_send, halo_recv, max_send, max_recv, load_sem, turn_sem,
):
    lx, ly, lz = shape
    rows = lx * ly
    groups = rows // LANES
    blocks = 8 // groups
    inner = lz // blocks
    x_edge, y_edge = 3 * ly, 3 * lx
    cons = qx.at[:, pl.ds(x_edge, rows), :]
    turned_y = qy.at[:, pl.ds(y_edge, rows), :]
    load = pltpu.make_async_copy(cons_hbm.reshape(5, rows, lz), cons, load_sem)
    load.start()
    me = [lax.axis_index(axis) for axis in AXES]
    count = sizes[0] * sizes[1] * sizes[2]
    plane = sizes[0] * sizes[2]
    place = (me[0] * sizes[1] + me[1]) * sizes[2] + me[2]
    is_root = me[0] + me[2] == 0
    roots = [{"gx": 0, "gy": r, "gz": 0} for r in range(sizes[1])]

    def beside(axis, up):
        return {AXES[axis]: lax.rem(me[axis] + (1 if up else sizes[axis] - 1), sizes[axis])}

    barrier = pltpu.get_barrier_semaphore()

    def greet(peer):
        pl.semaphore_signal(barrier, inc=1, device_id=peer, device_id_type=MESH)

    for axis in range(3):
        for up in (True, False):
            greet(beside(axis, up))

    @pl.when(is_root)
    def _():
        def tell(t, _):
            other = lax.rem(place + t, count)
            rest = other // sizes[2]
            greet({"gx": rest // sizes[1], "gy": rest % sizes[1], "gz": other % sizes[2]})
            return 0

        lax.fori_loop(1, count, tell, 0)

    for y in range(ly):
        pltpu.make_async_copy(cons_hbm.at[:, :, y, :], qy.at[:, pl.ds(y_edge + y * lx, lx), :], turn_sem).start()
    load.wait()

    best = [None] * 3
    for j in range(rows // 8):
        q = [qx[c, pl.ds(x_edge + 8 * j, 8), :] for c in range(5)]
        inv = 1.0 / q[0]
        vel = [q[d] * inv for d in (1, 2, 3)]
        kinetic = 0.5 * (vel[0] * vel[0] + vel[1] * vel[1] + vel[2] * vel[2])
        sound = jnp.sqrt((GAMMA * (GAMMA - 1.0)) * (q[4] * inv - kinetic))
        for d in range(3):
            value = jnp.abs(vel[d]) + sound
            best[d] = value if best[d] is None else jnp.maximum(best[d], value)
    lane = lax.broadcasted_iota(jnp.int32, (1, LANES), 1)
    local = [jnp.max(jnp.max(v, axis=0, keepdims=True), axis=1, keepdims=True) for v in best]
    mine[...] = jnp.where(lane == 0, local[0], jnp.where(lane == 1, local[1], local[2]))

    along = [
        Sweep(0, lx, ly // 8, qx, wx, kept_x),
        Sweep(1, ly, lx // 8, qy, wy, kept_y),
        Sweep(2, inner, 1, qz, wz, kept_z),
    ]
    @pl.when(is_root)
    def _():
        for axis in (0,):
            along[axis].inside()

    def halo(slot, src, dst, axis, up):
        return pltpu.make_async_remote_copy(
            src_ref=src, dst_ref=dst, send_sem=halo_send.at[slot], recv_sem=halo_recv.at[slot],
            device_id=beside(axis, up), device_id_type=MESH,
        )

    pl.semaphore_wait(barrier, 6 + sizes[1] - jnp.where(is_root, 1, 0))
    reports = []
    for r, root in enumerate(roots):
        slot = lax.rem(place - r * sizes[2] + count - 1, count)
        report = pltpu.make_async_remote_copy(
            src_ref=mine, dst_ref=theirs.at[slot], send_sem=max_send.at[r], recv_sem=max_recv.at[0],
            device_id=root, device_id_type=MESH,
        )
        pl.when(place != r * sizes[2])(report.start)
        reports.append(report)
    halos = [
        [
            halo(0, qx.at[:, pl.ds(rows, x_edge), :], qx.at[:, pl.ds(0, x_edge), :], 0, True),
            halo(1, qx.at[:, pl.ds(x_edge, x_edge), :], qx.at[:, pl.ds(x_edge + rows, x_edge), :], 0, False),
        ],
        [
            halo(2, qy.at[:, pl.ds(rows, y_edge), :], qy.at[:, pl.ds(0, y_edge), :], 1, True),
            halo(3, qy.at[:, pl.ds(y_edge, y_edge), :], qy.at[:, pl.ds(y_edge + rows, y_edge), :], 1, False),
        ],
        [halo(4, zsend.at[0], zh.at[0], 2, True), halo(5, zsend.at[1], zh.at[1], 2, False)],
    ]
    for copy in halos[0]:
        copy.start()
    for c in range(5):
        for g in range(groups):
            turned = jnp.transpose(qx[c, pl.ds(x_edge + g * LANES, LANES), :])
            for b in range(blocks):
                qz[c, pl.ds(24 + b * groups + g, inner, stride=8), :] = turned[b * inner:(b + 1) * inner]
            for k in range(3):
                zsend[0, pl.ds((3 * c + k) * groups + g, 1), :] = turned[lz - 3 + k:lz - 2 + k]
                zsend[1, pl.ds((3 * c + k) * groups + g, 1), :] = turned[k:k + 1]
    for copy in halos[2]:
        copy.start()
    pltpu.make_async_copy(turned_y, turned_y, turn_sem).wait()
    for copy in halos[1]:
        copy.start()

    def fill_y():
        for copy in halos[1]:
            copy.wait()
        along[1].outside()

    def fill_z():
        for copy in halos[2]:
            copy.wait()
        size = inner * 8
        for c in range(5):
            for k in range(3):
                low, high = 8 * k, 24 + size + 8 * k
                qz[c, low:low + groups, :] = zh[0, pl.ds((3 * c + k) * groups, groups), :]
                qz[c, low + groups:low + 8, :] = qz[c, size + 8 * k:size + 8 + 8 * k - groups, :]
                qz[c, high:high + 8 - groups, :] = qz[c, 24 + 8 * k + groups:32 + 8 * k, :]
                qz[c, high + 8 - groups:high + 8, :] = zh[1, pl.ds((3 * c + k) * groups, groups), :]
        along[2].outside()

    def fill_x():
        for copy in halos[0]:
            copy.wait()
        along[0].outside()

    def answer(peer):
        return pltpu.make_async_remote_copy(
            src_ref=top, dst_ref=top, send_sem=max_send.at[sizes[1]], recv_sem=max_recv.at[1],
            device_id=peer, device_id_type=MESH,
        )

    def bytes_of(refs, send, receive):
        return pltpu.make_async_remote_copy(
            src_ref=refs, dst_ref=refs, send_sem=max_send.at[send], recv_sem=max_recv.at[receive],
            device_id=beside(1, True), device_id_type=MESH,
        )

    @pl.when(is_root)
    def _():
        for axis in (2, 1):
            along[axis].inside()
        fill_y()
        bytes_of(theirs, 0, 0).wait_recv()
        top[...] = jnp.maximum(mine[...], jnp.max(theirs[...], axis=0))

        def tell(t, _):
            answer({"gx": t // sizes[2], "gy": me[1], "gz": t % sizes[2]}).start()
            return 0

        lax.fori_loop(1, plane, tell, 0)

    @pl.when(jnp.logical_not(is_root))
    def _():
        for axis in (1, 2, 0):
            along[axis].inside()
        fill_y()
        fill_z()
        answer(beside(1, True)).wait_recv()

    for r, report in enumerate(reports):
        pl.when(place != r * sizes[2])(report.wait_send)
    speed = [jnp.broadcast_to(top[0:1, d:d + 1], (8, LANES)) for d in range(3)]
    step = COURANT / (speed[0] * cells[0] + speed[1] * cells[1] + speed[2] * cells[2])
    factors[0] = 0.25 * speed[0]
    factors[1] = step * (cells[0] / 3.0)

    ry = lx // 8

    def place_y(j, c, value):
        y = jnp.maximum(j // ry - 1, 0)
        acc[c, pl.ds(8 * ly * (j % ry) + y, 8, stride=ly), :] = value

    def place_z(j, c, value):
        tz[c, rows_of(jnp.maximum(j - 1, 0)), :] = value

    def combine(axis, r, slots, put, unroll):
        sweep(axis, r, 0.25 * speed[axis], None, along[axis].kept, faces, put, 0, slots + 1, unroll)

    combine(1, ry, ly, place_y, 2)
    pl.when(is_root)(fill_z)
    combine(2, 1, inner, place_z, 3)
    scale = [(step * (cells[d] / 3.0))[:1] for d in range(3)]
    for c in range(5):
        for g in range(groups):
            parts = [tz[c, pl.ds(b * groups + g, inner, stride=8), :] for b in range(blocks)]
            turned = jnp.transpose(jnp.concatenate(parts, axis=0))
            here = pl.ds(g * LANES, LANES)
            held = qx[c, pl.ds(x_edge + g * LANES, LANES), :] + scale[1] * acc[c, here, :]
            acc[c, here, :] = held + scale[2] * turned
    fill_x()

    @pl.when(is_root)
    def _():
        bytes_of(theirs.at[pl.ds(0, plane - 1)], sizes[1], 1).wait_send()


def combine_kernel(shape, kept, acc, factors, out_hbm, out, faces, store_sem):
    lx, ly, lz = shape
    rx = ly // 8
    quarter, scale = factors[0], factors[1]

    def place(j, c, value):
        x = jnp.maximum(j // rx - 1, 0)
        here = rows_of(x * rx + j % rx)
        out[c, here, :] = acc[c, here, :] + value

    stores = []
    ends = [0, (6 * lx) // 16, (11 * lx) // 16, (14 * lx) // 16, lx]
    for m in range(4):
        low, high = ends[m], ends[m + 1]
        sweep(0, rx, quarter, scale, kept, faces, place, 0 if m == 0 else low + 1, high + 1, 2)
        part = pl.ds(low * ly, (high - low) * ly)
        stores.append(pltpu.make_async_copy(out.at[:, part, :], out_hbm.at[:, part, :], store_sem.at[m]))
        stores[-1].start()
    for store in stores:
        store.wait()


def solution(mesh):
    sizes = [mesh.shape[axis] for axis in AXES]
    count = sizes[0] * sizes[1] * sizes[2]

    def per_device(conserved):
        _, lx, ly, lz = conserved.shape
        shape = (lx, ly, lz)
        cells = [float(n * s) for n, s in zip(shape, sizes)]
        rows = lx * ly
        groups = rows // LANES
        inner = lz * groups // 8
        assert lz == LANES and rows % LANES == 0 and 8 % groups == 0 and lx % 8 == 0 and ly % 8 == 0
        def vmem(*dims):
            return pltpu.VMEM(dims, jnp.float32)

        def faces(count):
            return vmem(count, KEPT, 8, LANES)

        pads = [(lx + 6) * ly // 8, (ly + 6) * lx // 8, inner + 6]
        kept = [faces((lx + 1) * ly // 8), faces((ly + 1) * lx // 8), faces(inner + 1)]
        flux = vmem(max((lx + 2) * ly // 8, (ly + 2) * lx // 8, inner + 2), 5, 8, LANES)
        block = vmem(5, rows, lz)
        whole = pl.BlockSpec(memory_space=pltpu.VMEM)
        kept_x, acc, factors = pl.pallas_call(
            functools.partial(gather_kernel, sizes, cells, shape),
            name="gather",
            out_shape=[kept[0], block, vmem(2, 8, LANES)],
            in_specs=[pl.BlockSpec(memory_space=pltpu.HBM)],
            out_specs=[whole] * 3,
            scratch_shapes=[kept[1], kept[2], flux, vmem(5, 8 * inner, LANES)]
            + [vmem(5, 8 * n, LANES) for n in pads] + [vmem(n, 25, 8, LANES) for n in pads] + [
                vmem(2, 15 * groups, LANES),
                vmem(2, 15 * groups, LANES),
                vmem(1, LANES),
                vmem(1, LANES),
                vmem(count - 1, 1, LANES),
                pltpu.SemaphoreType.DMA((6,)),
                pltpu.SemaphoreType.DMA((6,)),
                pltpu.SemaphoreType.DMA((sizes[1] + 1,)),
                pltpu.SemaphoreType.DMA((2,)),
                pltpu.SemaphoreType.DMA,
                pltpu.SemaphoreType.DMA,
            ],
            compiler_params=pltpu.CompilerParams(
                collective_id=0, has_side_effects=True, vmem_limit_bytes=44 * 2**20
            ),
        )(pltpu.with_memory_space_constraint(conserved, pltpu.HBM))
        out = pl.pallas_call(
            functools.partial(combine_kernel, shape),
            name="combine",
            out_shape=jax.ShapeDtypeStruct((5, rows, lz), jnp.float32),
            in_specs=[whole] * 3,
            out_specs=pl.BlockSpec(memory_space=pl.ANY),
            scratch_shapes=[block, flux, pltpu.SemaphoreType.DMA((4,))],
            compiler_params=pltpu.CompilerParams(vmem_limit_bytes=16 * 2**20),
        )(kept_x, acc, factors)
        return out.reshape(conserved.shape)

    return jax.shard_map(
        per_device,
        mesh=mesh,
        in_specs=(P(None, "gx", "gy", "gz"),),
        out_specs=P(None, "gx", "gy", "gz"),
        check_vma=False,
    )
```
